32 devices in a mesh: ta: 4 (over x, core), ha: 4 (over z), wa: 2 (over y).
Axes of the slice: x: 2, y: 2, z: 4, core: 2. Of those that a mesh axis runs over, the one named last changes fastest.
Arguments:
- tokens: bfloat16 [1, 16, 32, 16, 1024], P(None, 'ta', 'ha', 'wa'), may hold values from -40 to 40
- norm_gain: float32 [4, 1024], replicated, may hold values from 0.25 to 1.75
- qkv_weight: bfloat16 [3, 1024, 3, 1024], P(None, None, None, 'ta'), may hold values from -0.1875 to 0.1875
- qk_gain: float32 [3, 2, 64], replicated, may hold values from 0.25 to 1.75
- out_weight: bfloat16 [3, 1024, 1024], P(None, 'ta'), may hold values from -0.1875 to 0.1875
- ffn_in: bfloat16 [1024, 2, 2048], P(None, None, 'ta'), may hold values from -0.1875 to 0.1875
- ffn_out: bfloat16 [2048, 1024], P('ta'), may hold values from -0.125 to 0.125
Outputs:
- layer_out: bfloat16 [1, 16, 32, 16, 1024], P(None, 'ta', 'ha', 'wa')
The draws below stay inside these ranges and needn't reach their ends.
All inputs are finite; a program needn't handle non-finite values.
Results may differ from the reference program's by a relative error of at most 0.015.
Values may be sent and summed in bfloat16 or wider, within the bound.
A program may use at most 192 MiB of HBM per device.

```python
import math
import jax
import jax.numpy as jnp
from jax import lax

D = 1024
HEAD_DIM = 64
FF = 2048
CLIPS = 1
ATTN_WIDTH = 1024
FRAMES = 16
HEIGHT = 32
WIDTH = 16
N_TA = 4


def draw_tokens(key, part):
    key_entries, key_column, key_row = jax.random.split(key, 3)
    extent = (CLIPS, FRAMES, HEIGHT, WIDTH, D)
    entries = jnp.clip(jax.random.normal(key_entries, extent, jnp.float32), -4.0, 4.0)
    column_scale = jnp.exp(jax.random.uniform(key_column, (D,), jnp.float32, math.log(0.3), math.log(3.0)))
    row_scale = jnp.exp(jax.random.uniform(key_row, extent[:4] + (1,), jnp.float32, math.log(0.5), math.log(2.0)))
    return (entries * column_scale * row_scale).astype(jnp.bfloat16)


def levels(key, shape, cuts, least, high):
    loudness, own = 1.0, jax.random.fold_in(key, 6)
    for axis_at, blocks in cuts:
        heights = jnp.exp(jax.random.uniform(jax.random.fold_in(own, axis_at), (blocks,), jnp.float32, least / len(cuts), high / len(cuts)))
        loudness = loudness * jnp.repeat(heights, shape[axis_at] // blocks).reshape([-1 if axis == axis_at else 1 for axis in range(len(shape))])
    return loudness


def gaussian(key, shape, spread, bound, shards=(), dtype=jnp.bfloat16):
    result = spread * jax.random.normal(key, shape, jnp.float32)
    if shards:
        result = result * levels(key, shape, shards, -0.22, 0.18)
    return jnp.clip(result, -bound, bound).astype(dtype)


def setup_inputs(seed: int = 0) -> dict:
    streams_of = jax.random.split(jax.random.key(seed), 8)
    return {
        "tokens": draw_tokens(jax.random.fold_in(streams_of[7], 71), 0),
        "norm_gain": jnp.clip(1.0 + 0.15 * jax.random.normal(streams_of[1], (4, D), jnp.float32), 0.25, 1.75),
        "qkv_weight": gaussian(streams_of[2], (3, D, 3, ATTN_WIDTH), D ** -0.5, 0.1875, ((3, 4),)),
        "qk_gain": jnp.clip(1.0 + 0.15 * jax.random.normal(streams_of[3], (3, 2, HEAD_DIM), jnp.float32), 0.25, 1.75),
        "out_weight": gaussian(streams_of[4], (3, ATTN_WIDTH, D), ATTN_WIDTH ** -0.5, 0.1875, ((1, 4),)),
        "ffn_in": gaussian(streams_of[5], (D, 2, FF), D ** -0.5, 0.1875, ((2, 4),)),
        "ffn_out": gaussian(streams_of[6], (FF, D), FF ** -0.5, 0.125, ((0, 4),)),
    }


def rms_norm(stream, gain_row):
    return stream * lax.rsqrt(lax.optimization_barrier(jnp.mean(stream * stream, axis=-1, keepdims=True)) + 1e-06) * gain_row

def head_norm(vectors, gain_row):
    return vectors * lax.rsqrt(lax.optimization_barrier(jnp.mean(vectors * vectors, axis=-1, keepdims=True)) + 1e-06) * gain_row

def grouped_product(left, right):
    inner = left.shape[-1]
    block = inner // N_TA
    left_blocks = left.reshape(-1, N_TA, block).astype(jnp.float32)
    right_blocks = right.reshape(N_TA, block, -1).astype(jnp.float32)
    parts = jnp.einsum('rgk,gkd->grd', left_blocks, right_blocks)
    rounded = lax.optimization_barrier(parts.astype(jnp.bfloat16))
    return lax.optimization_barrier(jnp.sum(rounded.astype(jnp.float32), axis=0))

def project(normed, weight_block, gain_pair):
    extent = normed.shape
    model_width = extent[-1]
    flat_qkv = jnp.dot(normed.reshape(-1, model_width), weight_block.reshape(model_width, -1), preferred_element_type=jnp.float32)
    head_count = weight_block.shape[-1] // HEAD_DIM
    flat_qkv = flat_qkv.reshape(extent[:4] + (3, head_count, HEAD_DIM))
    queries = head_norm(flat_qkv[..., 0, :, :], gain_pair[0])
    key_rows = head_norm(flat_qkv[..., 1, :, :], gain_pair[1])
    stacked = jnp.stack([queries, key_rows, flat_qkv[..., 2, :, :]], axis=4).astype(jnp.bfloat16)
    return stacked.reshape(extent[:4] + (3, head_count * HEAD_DIM))

def attend(packed, line_axis, causal):
    extent = packed.shape
    head_count = extent[-1] // HEAD_DIM
    split_shape = extent[:4] + (head_count, HEAD_DIM)
    queries = packed[..., 0, :].reshape(split_shape).astype(jnp.float32)
    key_rows = packed[..., 1, :].reshape(split_shape).astype(jnp.float32)
    values = packed[..., 2, :].reshape(split_shape).astype(jnp.float32)
    letters = 'cfyx'
    axis_letter = letters[line_axis]
    query_spec = letters.replace(axis_letter, 'q') + 'hd'
    key_spec = letters.replace(axis_letter, 'k') + 'hd'
    score_spec = letters.replace(axis_letter, '') + 'hqk'
    scores = jnp.einsum(query_spec + ',' + key_spec + '->' + score_spec, queries, key_rows) / math.sqrt(HEAD_DIM)
    exponentials = jnp.exp(scores)
    if causal:
        places = jnp.arange(extent[line_axis])
        exponentials = jnp.where(places[:, None] >= places[None, :], exponentials, jnp.zeros_like(exponentials))
    attn_probs = (exponentials / lax.optimization_barrier(jnp.sum(exponentials, axis=-1, keepdims=True))).astype(jnp.bfloat16)
    attended = jnp.einsum(score_spec + ',' + key_spec + '->' + query_spec, attn_probs.astype(jnp.float32), values)
    return attended.reshape(extent[:4] + (extent[-1],)).astype(jnp.bfloat16)

def attention_pass(stream, gain_row, weight_block, gain_pair, out_block, line_axis, causal):
    map_dim = 2 if line_axis == 1 else 1
    normed = rms_norm(stream, gain_row).astype(jnp.bfloat16)
    blocks = jnp.moveaxis(normed, map_dim, 0)

    def one_block(tile_block):
        restored = jnp.expand_dims(tile_block, map_dim)
        packed = project(restored, weight_block, gain_pair)
        attended = attend(packed, line_axis, causal)
        all_width = attended.shape[-1]
        delta_part = grouped_product(attended.reshape(-1, all_width), out_block)
        return jnp.squeeze(delta_part.reshape(restored.shape[:4] + (out_block.shape[1],)), map_dim)
    deltas = lax.map(one_block, blocks)
    return stream + jnp.moveaxis(deltas, 0, map_dim)

def mlp_block(stream, gain_row, ffn_in, ffn_out):
    normed = rms_norm(stream, gain_row).astype(jnp.bfloat16)
    blocks = jnp.moveaxis(normed, 1, 0)
    model_width = ffn_in.shape[0]
    hidden_width = ffn_in.shape[2]

    def one_frame(frame_tokens):
        flat_tokens = frame_tokens.reshape(-1, model_width)
        both_parts = jnp.dot(flat_tokens, ffn_in.reshape(model_width, -1), preferred_element_type=jnp.float32).reshape(-1, 2, hidden_width)
        hidden = (jax.nn.silu(both_parts[:, 0]) * both_parts[:, 1]).astype(jnp.bfloat16)
        return grouped_product(hidden, ffn_out).reshape(frame_tokens.shape)
    deltas = lax.map(one_frame, blocks)
    return stream + jnp.moveaxis(deltas, 0, 1)

def reference(tokens, norm_gain, qkv_weight, qk_gain, out_weight, ffn_in, ffn_out):
    stream = tokens.astype(jnp.float32)
    for pass_index, line_axis in ((0, 3), (1, 2), (2, 1)):
        stream = attention_pass(stream, norm_gain[pass_index], qkv_weight[pass_index], qk_gain[pass_index], out_weight[pass_index], line_axis, line_axis == 1)
    stream = mlp_block(stream, norm_gain[3], ffn_in, ffn_out)
    return stream.astype(jnp.bfloat16)
```

```python
import functools

import jax
import jax.numpy as jnp
from jax import lax
from jax.experimental import pallas as pl
from jax.experimental.pallas import tpu as pltpu
from jax.sharding import PartitionSpec as P

HEAD_DIM = 64
EPS = 1e-06
MESH = pl.DeviceIdType.MESH
F32 = jnp.float32
BF16 = jnp.bfloat16


def dot(a, b):
    return jnp.dot(a, b, preferred_element_type=F32)


def dot_t(a, b):
    return lax.dot_general(a, b, (((1,), (1,)), ((), ())), preferred_element_type=F32)


def mask_of(cond_rows, cond_cols):
    return cond_rows == cond_cols


def attend(queries, key_rows, values, mask):
    width = queries.shape[-1]
    lane_head = lax.broadcasted_iota(jnp.int32, (1, width), 1) // HEAD_DIM
    total = None
    for head in range(width // HEAD_DIM):
        pick = (lane_head == head).astype(F32).astype(BF16)
        scores = dot_t(queries * pick, key_rows)
        weights = jnp.where(mask, jnp.exp(scores), 0.0)
        probs = weights * (1.0 / jnp.sum(weights, axis=-1, keepdims=True))
        part = dot(probs.astype(BF16), values * pick)
        total = part if total is None else total + part
    return total.astype(BF16)


class Plan:
    def __init__(self, n, n_ta, frames, rows):
        self.n = n
        self.m = min(n, frames)
        self.unit = rows // self.m
        self.u = n_ta * self.m // n


def kernel(cfg, tok, gain, qkg, wq_h, wo_h, wi_h, wf_h, out, *s):
    n_ta, frames, height, width, plans = cfg
    (stream, gath, wq, wo, wi, wf, pk, a0, a1, res0, res1, att, pk2, att2, pbuf, prec, comb, xrec,
     wsem, ag_s, ag_r, s10, r10, s20, r20, s11, r11, s21, r21, rs_s, rs_r) = s
    rows = tok.shape[0]
    per_frame = height * width
    aw = wo.shape[1]
    me = lax.axis_index("ta")
    core, chip = lax.rem(me, 2), lax.div(me, 2)

    def block_at(k):
        return lax.rem(chip + lax.div(k, 2), 2) * 2 + lax.rem(core + lax.rem(k, 2), 2)

    partner = block_at(1)
    remote = block_at(2)
    pair_last = block_at(3)

    copies = []
    for at in range(3):
        copies.append(pltpu.make_async_copy(wq_h.at[at], wq.at[at], wsem.at[at]))
        copies.append(pltpu.make_async_copy(wo_h.at[at], wo.at[at], wsem.at[3 + at]))
    copies.append(pltpu.make_async_copy(wi_h, wi, wsem.at[6]))
    copies.append(pltpu.make_async_copy(wf_h, wf, wsem.at[7]))
    for copy in copies:
        copy.start()

    barrier = pltpu.get_barrier_semaphore()
    greets = 0
    for other in (partner, remote):
        pl.semaphore_signal(barrier, inc=1, device_id={"ta": other}, device_id_type=MESH)
        greets += 1
    for axis, plan in plans:
        here = lax.axis_index(axis)
        for step in range(1, plan.n):
            other = lax.rem(here + step, plan.n)
            pl.semaphore_signal(barrier, inc=1, device_id={axis: other}, device_id_type=MESH)
            greets += 1

    def remote_copy(src, dst, send, recv, axis, other):
        return pltpu.make_async_remote_copy(
            src_ref=src, dst_ref=dst, send_sem=send, recv_sem=recv,
            device_id={axis: other}, device_id_type=MESH)

    def norm_own(p):
        x = stream[...]
        scale = lax.rsqrt(jnp.mean(x * x, axis=-1, keepdims=True) + EPS)
        gath[p, me] = (x * scale * gain[p:p + 1, :]).astype(BF16)

    def ag_copy(p, slot):
        block = me if slot < 2 else remote
        other = remote if slot == 1 else partner
        ref = gath.at[p, block]
        return remote_copy(ref, ref, ag_s.at[p, slot], ag_r.at[p, slot], "ta", other)

    def ag_start(p):
        ag_copy(p, 1).start()
        ag_copy(p, 0).start()

    def ag_wait(p, k):
        @pl.when(k == 1)
        def _():
            ag_copy(p, 0).wait_recv()

        @pl.when(k == 2)
        def _():
            ag_copy(p, 1).wait_recv()
            ag_copy(p, 2).start()

        @pl.when(k == 3)
        def _():
            ag_copy(p, 2).wait_recv()

    lane_a = lax.broadcasted_iota(jnp.int32, (aw, aw), 0) // HEAD_DIM
    lane_b = lax.broadcasted_iota(jnp.int32, (aw, aw), 1) // HEAD_DIM
    ones = (lane_a == lane_b).astype(F32).astype(BF16)

    def head_norm(x, row):
        square = x * x
        high = square.astype(BF16)
        low = (square - high.astype(F32)).astype(BF16)
        mean = (dot(high, ones) + dot(low, ones)) * (1.0 / HEAD_DIM)
        return x * lax.rsqrt(mean + EPS) * qkg[row:row + 1, :]

    def project(p, b):
        flat = dot(gath[p, b], wq[p])
        queries = (head_norm(flat[:, :aw], 2 * p) * (HEAD_DIM ** -0.5)).astype(BF16)
        key_rows = head_norm(flat[:, aw:2 * aw], 2 * p + 1).astype(BF16)
        return queries, key_rows, flat[:, 2 * aw:].astype(BF16)

    def rs_copy(p, slot):
        if slot == 0:
            return remote_copy(pbuf.at[p, 1], prec.at[p, 0], rs_s.at[p, 0], rs_r.at[p, 0], "ta", partner)
        if slot == 1:
            return remote_copy(pbuf.at[p, 3], prec.at[p, 1], rs_s.at[p, 1], rs_r.at[p, 1], "ta", partner)
        return remote_copy(comb.at[p], xrec.at[p], rs_s.at[p, 2], rs_r.at[p, 2], "ta", remote)

    def rs_put(p, k, part):
        pbuf[p, k] = part.astype(BF16)

        @pl.when(k == 1)
        def _():
            rs_copy(p, 0).start()

        @pl.when(k == 3)
        def _():
            rs_copy(p, 1).start()

    def rs_combine(p):
        rs_copy(p, 1).wait_recv()
        comb[p] = (pbuf[p, 2].astype(F32) + prec[p, 1].astype(F32)).astype(BF16)
        rs_copy(p, 2).start()

    def rs_total(p):
        rs_copy(p, 0).wait_recv()
        near = pbuf[p, 0].astype(F32) + prec[p, 0].astype(F32)
        rs_copy(p, 2).wait_recv()
        return stream[...] + (near + xrec[p].astype(F32))

    stream[...] = tok[...].astype(F32)
    norm_own(0)
    pl.semaphore_wait(barrier, greets)
    ag_start(0)

    sends = []
    for p in (0, 1):
        axis, plan = plans[p]
        n, m, unit, groups = plan.n, plan.m, plan.unit, plan.u
        here = lax.axis_index(axis)
        abuf, res = ((a0, res0), (a1, res1))[p]
        s1, r1, s2, r2 = ((s10, r10, s20, r20), (s11, r11, s21, r21))[p]
        if p:
            norm_own(p)
            ag_start(p)
        copies[2 * p].wait()

        def unit_copy(b, j, p=p, axis=axis, m=m, unit=unit, groups=groups, here=here, abuf=abuf, s1=s1, r1=r1):
            owner = j + m * lax.div(b, groups)
            u = lax.rem(b, groups)
            return owner, u, remote_copy(
                pk.at[p, b, pl.ds(j * unit, unit)], abuf.at[u, here], s1.at[b, j], r1.at[u, here], axis, owner)

        def first(k, _, p=p, m=m, unit=unit, here=here, abuf=abuf, unit_copy=unit_copy):
            b = block_at(k)
            ag_wait(p, k)
            queries, key_rows, values = project(p, b)
            pk[p, b, :, 0:aw] = queries
            pk[p, b, :, aw:2 * aw] = key_rows
            pk[p, b, :, 2 * aw:3 * aw] = values
            for j in range(m):
                owner, u, copy = unit_copy(b, j)

                @pl.when(owner != here)
                def _():
                    copy.start()

                @pl.when(owner == here)
                def _():
                    abuf[u, here] = pk[p, b, j * unit:(j + 1) * unit, :]
            return 0

        lax.fori_loop(0, n_ta, first, 0)

        size = n * unit
        if p == 0:
            line_of = lambda at: lax.div(lax.rem(at, unit), width)
        else:
            line_of = lambda at: lax.div(lax.rem(at, unit), per_frame) * width + lax.rem(at, width)
        mask = line_of(lax.broadcasted_iota(jnp.int32, (size, 1), 0)) == line_of(
            lax.broadcasted_iota(jnp.int32, (1, size), 1))

        def back_copy(u, other, p=p, axis=axis, m=m, unit=unit, groups=groups, here=here, res=res, s2=s2, r2=r2):
            j = lax.rem(here, m)
            b = u + groups * lax.div(here, m)
            return remote_copy(
                res.at[u, other], att.at[p, b, pl.ds(pl.multiple_of(j * unit, unit), unit)],
                s2.at[u, other], r2.at[b, j], axis, other)

        def second(k, _, p=p, axis=axis, n=n, m=m, unit=unit, groups=groups, here=here, abuf=abuf, res=res,
                   r1=r1, s1=s1, mask=mask, size=size, back_copy=back_copy):
            u = lax.rem(block_at(k), groups)
            for step in range(1, n):
                source = lax.rem(here + step, n)
                remote_copy(abuf.at[u, source], abuf.at[u, source], s1.at[0, 0], r1.at[u, source],
                            axis, source).wait_recv()
            done = attend(
                abuf[u, :, :, 0:aw].reshape(size, aw),
                abuf[u, :, :, aw:2 * aw].reshape(size, aw),
                abuf[u, :, :, 2 * aw:3 * aw].reshape(size, aw),
                mask,
            )
            res[u] = done.reshape(n, unit, aw)
            for step in range(1, n):
                back_copy(u, lax.rem(here + step, n)).start()
            j = lax.rem(here, m)
            b = u + groups * lax.div(here, m)
            att[p, b, pl.ds(pl.multiple_of(j * unit, unit), unit)] = res[u, here]
            return 0

        lax.fori_loop(0, groups, second, 0)
        copies[2 * p + 1].wait()

        def third(i, _, p=p, axis=axis, m=m, unit=unit, groups=groups, here=here, s2=s2, r2=r2):
            k = n_ta - 1 - i
            b = block_at(k)
            for j in range(m):
                owner = j + m * lax.div(b, groups)

                @pl.when(owner != here)
                def _():
                    ref = att.at[p, b, pl.ds(j * unit, unit)]
                    remote_copy(ref, ref, s2.at[0, 0], r2.at[b, j], axis, owner).wait_recv()
            rs_put(p, k, dot(att[p, b], wo[p]))

            @pl.when(k == 2)
            def _():
                rs_combine(p)
            return 0

        lax.fori_loop(0, n_ta, third, 0)
        stream[...] = rs_total(p)

        def drain(unit_copy=unit_copy, back_copy=back_copy, n=n, m=m, groups=groups, here=here):
            for b in range(n_ta):
                for j in range(m):
                    owner, _, copy = unit_copy(b, j)

                    @pl.when(owner != here)
                    def _():
                        copy.wait_send()
            for u in range(groups):
                for step in range(1, n):
                    back_copy(u, lax.rem(here + step, n)).wait_send()

        sends.append(drain)

    p = 2
    norm_own(p)
    ag_start(p)
    copies[2 * p].wait()

    def time_first(k, _):
        b = block_at(k)
        ag_wait(p, k)
        queries, key_rows, values = project(p, b)
        at = pl.ds(b * frames, frames)
        pk2[at, :, 0:aw] = queries.reshape(frames, per_frame, aw)
        pk2[at, :, aw:2 * aw] = key_rows.reshape(frames, per_frame, aw)
        pk2[at, :, 2 * aw:3 * aw] = values.reshape(frames, per_frame, aw)
        return 0

    lax.fori_loop(0, n_ta, time_first, 0)
    every = n_ta * frames
    some = 16
    size = every * some
    i_at = lax.broadcasted_iota(jnp.int32, (size, 1), 0)
    j_at = lax.broadcasted_iota(jnp.int32, (1, size), 1)
    causal = (lax.rem(i_at, some) == lax.rem(j_at, some)) & (lax.div(i_at, some) >= lax.div(j_at, some))

    def time_second(g, _):
        at = pl.ds(pl.multiple_of(g * some, some), some)
        done = attend(
            pk2[:, at, 0:aw].reshape(size, aw),
            pk2[:, at, aw:2 * aw].reshape(size, aw),
            pk2[:, at, 2 * aw:3 * aw].reshape(size, aw),
            causal,
        )
        att2[:, at, :] = done.reshape(every, some, aw)
        return 0

    lax.fori_loop(0, per_frame // some, time_second, 0)
    copies[2 * p + 1].wait()

    def time_third(i, _):
        k = n_ta - 1 - i
        b = block_at(k)
        rs_put(p, k, dot(att2[pl.ds(b * frames, frames)].reshape(rows, aw), wo[p]))

        @pl.when(k == 2)
        def _():
            rs_combine(p)
        return 0

    lax.fori_loop(0, n_ta, time_third, 0)
    stream[...] = rs_total(p)

    norm_own(3)
    ag_start(3)
    copies[6].wait()
    copies[7].wait()
    half = wf.shape[0]

    def mlp(k, _):
        b = block_at(k)
        ag_wait(3, k)
        both = dot(gath[3, b], wi[...])
        gate, up = both[:, :half], both[:, half:]
        hidden = (gate / (1.0 + jnp.exp(-gate)) * up).astype(BF16)
        rs_put(3, k, dot(hidden, wf[...]))
        return 0

    lax.fori_loop(0, n_ta, mlp, 0)
    rs_combine(3)
    out[...] = rs_total(3).astype(BF16)

    for drain in sends:
        drain()
    for p in range(4):
        for slot in range(3):
            ag_copy(p, slot).wait_send()
            rs_copy(p, slot).wait_send()


def local(sizes, tokens, norm_gain, qkv_weight, qk_gain, out_weight, ffn_in, ffn_out):
    n_ta, n_ha, n_wa = sizes
    extent = tokens.shape
    clips, frames, height, width, model = extent
    rows = clips * frames * height * width
    aw = qkv_weight.shape[-1]
    half = ffn_in.shape[-1]
    plans = (("wa", Plan(n_wa, n_ta, frames, rows)), ("ha", Plan(n_ha, n_ta, frames, rows)))
    cfg = (n_ta, frames, height, width, plans)
    heads = aw // HEAD_DIM
    gains = jnp.tile(qk_gain.reshape(-1, HEAD_DIM), (1, heads))
    dma = pltpu.SemaphoreType.DMA
    vm = pltpu.VMEM
    scratch = [
        vm((rows, model), F32),
        vm((4, n_ta, rows, model), BF16),
        vm((3, model, 3 * aw), BF16),
        vm((3, aw, model), BF16),
        vm((model, 2 * half), BF16),
        vm((half, model), BF16),
        vm((2, n_ta, rows, 3 * aw), BF16),
    ]
    for width_of in (3 * aw, aw):
        for _, plan in plans:
            scratch.append(vm((plan.u, plan.n, plan.unit, width_of), BF16))
    scratch += [
        vm((2, n_ta, rows, aw), BF16),
        vm((n_ta * frames, height * width, 3 * aw), BF16),
        vm((n_ta * frames, height * width, aw), BF16),
        vm((4, n_ta, rows, model), BF16),
        vm((4, 2, rows, model), BF16),
        vm((4, rows, model), BF16),
        vm((4, rows, model), BF16),
        dma((8,)),
        dma((4, 3)),
        dma((4, 3)),
    ]
    for _, plan in plans:
        scratch += [
            dma((n_ta, plan.m)),
            dma((plan.u, plan.n)),
            dma((plan.u, plan.n)),
            dma((n_ta, plan.m)),
        ]
    scratch += [dma((4, 3)), dma((4, 3))]
    vmem = pl.BlockSpec(memory_space=pltpu.VMEM)
    anyw = pl.BlockSpec(memory_space=pl.ANY)
    result = pl.pallas_call(
        functools.partial(kernel, cfg),
        out_shape=jax.ShapeDtypeStruct((rows, model), BF16),
        in_specs=[vmem, vmem, vmem, anyw, anyw, anyw, anyw],
        out_specs=vmem,
        scratch_shapes=scratch,
        compiler_params=pltpu.CompilerParams(
            collective_id=0, has_side_effects=True, vmem_limit_bytes=67043328),
        name="axial_layer",
    )(
        tokens.reshape(rows, model),
        norm_gain,
        gains,
        qkv_weight.reshape(3, model, 3 * aw),
        out_weight,
        ffn_in.reshape(model, 2 * half),
        ffn_out,
    )
    return result.reshape(extent)


def solution(mesh):
    sizes = tuple(mesh.shape[name] for name in ("ta", "ha", "wa"))
    return jax.shard_map(
        functools.partial(local, sizes),
        mesh=mesh,
        in_specs=(
            P(None, "ta", "ha", "wa", None),
            P(),
            P(None, None, None, "ta"),
            P(),
            P(None, "ta", None),
            P(None, None, "ta"),
            P("ta", None),
        ),
        out_specs=P(None, "ta", "ha", "wa", None),
        check_vma=False,
    )
```

```python
import functools

import jax
import jax.numpy as jnp
from jax import lax
from jax.experimental import pallas as pl
from jax.experimental.pallas import tpu as pltpu
from jax.sharding import PartitionSpec as P

HEAD_DIM = 64
CHUNKS = 2
EPS = 1e-06
MESH = pl.DeviceIdType.MESH
F32 = jnp.float32
BF16 = jnp.bfloat16


def dot(a, b):
    return jnp.dot(a, b, preferred_element_type=F32)


def dot_t(a, b):
    return lax.dot_general(a, b, (((1,), (1,)), ((), ())), preferred_element_type=F32)


def attend(queries, key_rows, values, mask):
    width = queries.shape[-1]
    lane_head = lax.broadcasted_iota(jnp.int32, (1, width), 1) // HEAD_DIM
    total = None
    for head in range(width // HEAD_DIM):
        pick = (lane_head == head).astype(F32).astype(BF16)
        scores = dot_t(queries * pick, key_rows)
        weights = jnp.where(mask, jnp.exp(scores), 0.0)
        probs = weights * (1.0 / jnp.sum(weights, axis=-1, keepdims=True))
        part = dot(probs.astype(BF16), values * pick)
        total = part if total is None else total + part
    return total.astype(BF16)


class Plan:
    def __init__(self, n, n_ta, frames, rows):
        self.n = n
        self.m = frames
        self.unit = rows // frames
        self.low = min(n, frames)
        self.q = frames // self.low
        self.blocks = n_ta * frames // max(n, frames)
        self.u = self.blocks * self.q


def kernel(cfg, tok, gain, qkg, wq_h, wo_h, wi_h, wf_h, out, *s):
    n_ta, frames, height, width, plans = cfg
    (stream, gath, wq, wo, wi, wf, pk, a0, a1, res0, res1, att, pk2, att2, pbuf, prec, comb, xrec,
     wsem, ag_s, ag_r, s10, r10, s20, r20, s11, r11, s21, r21, rs_s, rs_r) = s
    rows = tok.shape[0]
    per_frame = height * width
    aw = wo.shape[1]
    me = lax.axis_index("ta")
    core, chip = lax.rem(me, 2), lax.div(me, 2)

    def block_at(k):
        return lax.rem(chip + lax.div(k, 2), 2) * 2 + lax.rem(core + lax.rem(k, 2), 2)

    piece = rows // CHUNKS
    wide = lambda c: pl.ds(pl.multiple_of(c * piece, piece), piece)
    steps = n_ta * CHUNKS
    early = 2 * CHUNKS

    def arrival(i):
        late = i - early
        k = jnp.where(i < early, lax.div(i, CHUNKS), 2 + lax.rem(late, 2))
        c = jnp.where(i < early, lax.rem(i, CHUNKS), lax.div(late, 2))
        return k, c

    def departure(i):
        rest = i - early
        k = jnp.where(i < early, 3 - lax.rem(i, 2), 1 - lax.div(rest, CHUNKS))
        c = jnp.where(i < early, lax.div(i, 2), lax.rem(rest, CHUNKS))
        return k, c

    partner = block_at(1)
    remote = block_at(2)
    pair_last = block_at(3)

    copies = []
    for at in range(3):
        copies.append([
            pltpu.make_async_copy(wq_h.at[at, j], wq.at[at, :, j * aw:(j + 1) * aw], wsem.at[at, j])
            for j in range(3)])
        copies.append([pltpu.make_async_copy(wo_h.at[at], wo.at[at], wsem.at[at, 3])])
    copies.append([pltpu.make_async_copy(wi_h, wi, wsem.at[3, 0])])
    copies.append([pltpu.make_async_copy(wf_h, wf, wsem.at[3, 1])])
    for group in copies:
        for copy in group:
            copy.start()

    def ready(at):
        for copy in copies[at]:
            copy.wait()

    barrier = pltpu.get_barrier_semaphore()
    greets = 0
    for other in (partner, remote):
        pl.semaphore_signal(barrier, inc=1, device_id={"ta": other}, device_id_type=MESH)
        greets += 1
    for axis, plan in plans:
        here = lax.axis_index(axis)
        for step in range(1, plan.n):
            other = lax.rem(here + step, plan.n)
            pl.semaphore_signal(barrier, inc=1, device_id={axis: other}, device_id_type=MESH)
            greets += 1

    def remote_copy(src, dst, send, recv, axis, other):
        return pltpu.make_async_remote_copy(
            src_ref=src, dst_ref=dst, send_sem=send, recv_sem=recv,
            device_id={axis: other}, device_id_type=MESH)

    def norm_own(p, c):
        x = stream[wide(c), :]
        scale = lax.rsqrt(jnp.mean(x * x, axis=-1, keepdims=True) + EPS)
        gath[p, me, wide(c)] = (x * scale * gain[p:p + 1, :]).astype(BF16)

    def ag_copy(p, slot, c):
        block = me if slot < 2 else remote
        other = remote if slot == 1 else partner
        ref = gath.at[p, block, wide(c)]
        return remote_copy(ref, ref, ag_s.at[p, slot, c], ag_r.at[p, slot, c], "ta", other)

    def ag_start(p, c):
        ag_copy(p, 1, c).start()
        ag_copy(p, 0, c).start()

    def ag_wait(p, k, c):
        @pl.when(k == 1)
        def _():
            ag_copy(p, 0, c).wait_recv()

        @pl.when(k == 2)
        def _():
            ag_copy(p, 1, c).wait_recv()
            ag_copy(p, 2, c).start()

        @pl.when(k == 3)
        def _():
            ag_copy(p, 2, c).wait_recv()

    lane_a = lax.broadcasted_iota(jnp.int32, (aw, aw), 0) // HEAD_DIM
    lane_b = lax.broadcasted_iota(jnp.int32, (aw, aw), 1) // HEAD_DIM
    ones = (lane_a == lane_b).astype(F32).astype(BF16)

    def head_norm(x, row):
        square = x * x
        high = square.astype(BF16)
        low = (square - high.astype(F32)).astype(BF16)
        mean = (dot(high, ones) + dot(low, ones)) * (1.0 / HEAD_DIM)
        return x * lax.rsqrt(mean + EPS) * qkg[row:row + 1, :]

    def project(p, b, c):
        flat = dot(gath[p, b, wide(c)], wq[p])
        queries = (head_norm(flat[:, :aw], 2 * p) * (HEAD_DIM ** -0.5)).astype(BF16)
        key_rows = head_norm(flat[:, aw:2 * aw], 2 * p + 1).astype(BF16)
        return queries, key_rows, flat[:, 2 * aw:].astype(BF16)

    def rs_copy(p, slot, c):
        send, recv = rs_s.at[p, slot, c], rs_r.at[p, slot, c]
        if slot == 2:
            return remote_copy(comb.at[p, wide(c)], xrec.at[p, wide(c)], send, recv, "ta", remote)
        return remote_copy(pbuf.at[p, 2 * slot + 1, wide(c)], prec.at[p, slot, wide(c)], send, recv, "ta", partner)

    def rs_put(p, k, c, part):
        pbuf[p, k, wide(c)] = part.astype(BF16)

        @pl.when(k == 1)
        def _():
            rs_copy(p, 0, c).start()

        @pl.when(k == 3)
        def _():
            rs_copy(p, 1, c).start()

    def rs_combine(p, c):
        rs_copy(p, 1, c).wait_recv()
        comb[p, wide(c)] = (pbuf[p, 2, wide(c)].astype(F32) + prec[p, 1, wide(c)].astype(F32)).astype(BF16)
        rs_copy(p, 2, c).start()

    def rs_total(p, c):
        rs_copy(p, 0, c).wait_recv()
        near = pbuf[p, 0, wide(c)].astype(F32) + prec[p, 0, wide(c)].astype(F32)
        rs_copy(p, 2, c).wait_recv()
        return stream[wide(c), :] + (near + xrec[p, wide(c)].astype(F32))

    def turn(p):
        for c in range(CHUNKS):
            stream[wide(c), :] = rs_total(p, c)
            norm_own(p + 1, c)
            ag_start(p + 1, c)

    stream[...] = tok[...].astype(F32)
    norm_own(0, 0)
    pl.semaphore_wait(barrier, greets)
    ag_start(0, 0)
    for c in range(1, CHUNKS):
        norm_own(0, c)
        ag_start(0, c)

    sends = []
    for p in (0, 1):
        axis, plan = plans[p]
        n, m, unit, groups, low, fold, span = plan.n, plan.m, plan.unit, plan.u, plan.low, plan.q, plan.blocks
        here = lax.axis_index(axis)
        abuf, res = ((a0, res0), (a1, res1))[p]
        s1, r1, s2, r2 = ((s10, r10, s20, r20), (s11, r11, s21, r21))[p]
        ready(2 * p)

        def owner_of(b, j, m=m, low=low, span=span):
            return lax.rem(j, low) + m * lax.div(b, span)

        def place(j, unit=unit):
            return pl.ds(pl.multiple_of(j * unit, unit), unit)

        def unit_copy(b, j, p=p, axis=axis, low=low, fold=fold, span=span, here=here, abuf=abuf, s1=s1, r1=r1,
                      owner_of=owner_of, place=place):
            owner = owner_of(b, j)
            u = lax.rem(b, span) * fold + lax.div(j, low)
            return owner, u, remote_copy(
                pk.at[p, b, place(j)], abuf.at[u, here], s1.at[b, j], r1.at[u, here], axis, owner)

        def first(i, _, p=p, m=m, here=here, abuf=abuf, unit_copy=unit_copy, place=place):
            k, c = arrival(i)
            b = block_at(k)
            ag_wait(p, k, c)
            queries, key_rows, values = project(p, b, c)
            pk[p, b, wide(c), 0:aw] = queries
            pk[p, b, wide(c), aw:2 * aw] = key_rows
            pk[p, b, wide(c), 2 * aw:3 * aw] = values
            for at in range(m // CHUNKS):
                j = c * (m // CHUNKS) + at
                owner, u, copy = unit_copy(b, j)

                @pl.when(owner != here)
                def _():
                    copy.start()

                @pl.when(owner == here)
                def _():
                    abuf[u, here] = pk[p, b, place(j), :]
            return 0

        lax.fori_loop(0, steps, first, 0)

        size = n * unit
        if p == 0:
            line_of = lambda at: lax.div(lax.rem(at, unit), width)
        else:
            line_of = lambda at: lax.div(lax.rem(at, unit), per_frame) * width + lax.rem(at, width)
        mask = line_of(lax.broadcasted_iota(jnp.int32, (size, 1), 0)) == line_of(
            lax.broadcasted_iota(jnp.int32, (1, size), 1))

        def home(u, m=m, low=low, fold=fold, span=span, here=here):
            return lax.div(u, fold) + span * lax.div(here, m), lax.rem(here, low) + low * lax.rem(u, fold)

        def back_copy(u, other, p=p, axis=axis, res=res, s2=s2, r2=r2, home=home, place=place):
            b, j = home(u)
            return remote_copy(
                res.at[u, other], att.at[p, b, place(j)], s2.at[u, other], r2.at[b, j], axis, other)

        def second(i, _, p=p, axis=axis, n=n, unit=unit, fold=fold, span=span, here=here, abuf=abuf, res=res,
                   r1=r1, s1=s1, mask=mask, size=size, back_copy=back_copy, home=home, place=place):
            k, sub = arrival(i) if fold == CHUNKS else (lax.div(i, fold), lax.rem(i, fold))
            u = lax.rem(block_at(k), span) * fold + sub
            for step in range(1, n):
                source = lax.rem(here + step, n)
                remote_copy(abuf.at[u, source], abuf.at[u, source], s1.at[0, 0], r1.at[u, source],
                            axis, source).wait_recv()
            done = attend(
                abuf[u, :, :, 0:aw].reshape(size, aw),
                abuf[u, :, :, aw:2 * aw].reshape(size, aw),
                abuf[u, :, :, 2 * aw:3 * aw].reshape(size, aw),
                mask,
            )
            res[u] = done.reshape(n, unit, aw)
            for step in range(1, n):
                back_copy(u, lax.rem(here + step, n)).start()
            b, j = home(u)
            att[p, b, place(j)] = res[u, here]
            return 0

        lax.fori_loop(0, groups, second, 0)
        ready(2 * p + 1)

        def third(i, _, p=p, axis=axis, m=m, here=here, s2=s2, r2=r2, owner_of=owner_of, place=place):
            k, c = departure(i)
            b = block_at(k)
            for at in range(m // CHUNKS):
                j = c * (m // CHUNKS) + at
                owner = owner_of(b, j)

                @pl.when(owner != here)
                def _():
                    ref = att.at[p, b, place(j)]
                    remote_copy(ref, ref, s2.at[0, 0], r2.at[b, j], axis, owner).wait_recv()
            rs_put(p, k, c, dot(att[p, b, wide(c)], wo[p]))

            @pl.when(k == 2)
            def _():
                rs_combine(p, c)
            return 0

        lax.fori_loop(0, steps, third, 0)
        turn(p)

        def drain(unit_copy=unit_copy, back_copy=back_copy, n=n, m=m, groups=groups, here=here):
            for b in range(n_ta):
                for j in range(m):
                    owner, _, copy = unit_copy(b, j)

                    @pl.when(owner != here)
                    def _():
                        copy.wait_send()
            for u in range(groups):
                for step in range(1, n):
                    back_copy(u, lax.rem(here + step, n)).wait_send()

        sends.append(drain)

    p = 2
    some_frames = frames // CHUNKS
    ready(2 * p)

    def time_first(i, _):
        k, c = arrival(i)
        b = block_at(k)
        ag_wait(p, k, c)
        queries, key_rows, values = project(p, b, c)
        at = pl.ds(b * frames + c * some_frames, some_frames)
        pk2[at, :, 0:aw] = queries.reshape(some_frames, per_frame, aw)
        pk2[at, :, aw:2 * aw] = key_rows.reshape(some_frames, per_frame, aw)
        pk2[at, :, 2 * aw:3 * aw] = values.reshape(some_frames, per_frame, aw)
        return 0

    lax.fori_loop(0, steps, time_first, 0)
    every = n_ta * frames
    some = 16
    size = every * some
    i_at = lax.broadcasted_iota(jnp.int32, (size, 1), 0)
    j_at = lax.broadcasted_iota(jnp.int32, (1, size), 1)
    causal = (lax.rem(i_at, some) == lax.rem(j_at, some)) & (lax.div(i_at, some) >= lax.div(j_at, some))

    def time_second(g, _):
        at = pl.ds(pl.multiple_of(g * some, some), some)
        done = attend(
            pk2[:, at, 0:aw].reshape(size, aw),
            pk2[:, at, aw:2 * aw].reshape(size, aw),
            pk2[:, at, 2 * aw:3 * aw].reshape(size, aw),
            causal,
        )
        att2[:, at, :] = done.reshape(every, some, aw)
        return 0

    lax.fori_loop(0, per_frame // some, time_second, 0)
    ready(2 * p + 1)

    def time_third(i, _):
        k, c = departure(i)
        b = block_at(k)
        at = pl.ds(b * frames + c * some_frames, some_frames)
        rs_put(p, k, c, dot(att2[at].reshape(piece, aw), wo[p]))

        @pl.when(k == 2)
        def _():
            rs_combine(p, c)
        return 0

    lax.fori_loop(0, steps, time_third, 0)
    turn(p)

    ready(6)
    ready(7)
    half = wf.shape[0]

    def mlp(i, _):
        k, c = arrival(i)
        b = block_at(k)
        ag_wait(3, k, c)
        both = dot(gath[3, b, wide(c)], wi[...])
        gate, up = both[:, :half], both[:, half:]
        hidden = (gate / (1.0 + jnp.exp(-gate)) * up).astype(BF16)
        rs_put(3, k, c, dot(hidden, wf[...]))

        @pl.when((k == 2) & (c > 0))
        def _():
            rs_combine(3, c - 1)
        return 0

    lax.fori_loop(0, steps, mlp, 0)
    rs_combine(3, CHUNKS - 1)
    for c in range(CHUNKS):
        out[wide(c), :] = rs_total(3, c).astype(BF16)

    for drain in sends:
        drain()
    for p in range(4):
        for slot in range(3):
            for c in range(CHUNKS):
                ag_copy(p, slot, c).wait_send()
                rs_copy(p, slot, c).wait_send()


def local(sizes, tokens, norm_gain, qkv_weight, qk_gain, out_weight, ffn_in, ffn_out):
    n_ta, n_ha, n_wa = sizes
    extent = tokens.shape
    clips, frames, height, width, model = extent
    rows = clips * frames * height * width
    aw = qkv_weight.shape[-1]
    half = ffn_in.shape[-1]
    plans = (("wa", Plan(n_wa, n_ta, frames, rows)), ("ha", Plan(n_ha, n_ta, frames, rows)))
    cfg = (n_ta, frames, height, width, plans)
    heads = aw // HEAD_DIM
    gains = jnp.tile(qk_gain.reshape(-1, HEAD_DIM), (1, heads))
    dma = pltpu.SemaphoreType.DMA
    vm = pltpu.VMEM
    scratch = [
        vm((rows, model), F32),
        vm((4, n_ta, rows, model), BF16),
        vm((3, model, 3 * aw), BF16),
        vm((3, aw, model), BF16),
        vm((model, 2 * half), BF16),
        vm((half, model), BF16),
        vm((2, n_ta, rows, 3 * aw), BF16),
    ]
    for width_of in (3 * aw, aw):
        for _, plan in plans:
            scratch.append(vm((plan.u, plan.n, plan.unit, width_of), BF16))
    scratch += [
        vm((2, n_ta, rows, aw), BF16),
        vm((n_ta * frames, height * width, 3 * aw), BF16),
        vm((n_ta * frames, height * width, aw), BF16),
        vm((4, n_ta, rows, model), BF16),
        vm((4, 2, rows, model), BF16),
        vm((4, rows, model), BF16),
        vm((4, rows, model), BF16),
        dma((4, 4)),
        dma((4, 3, CHUNKS)),
        dma((4, 3, CHUNKS)),
    ]
    for _, plan in plans:
        scratch += [
            dma((n_ta, plan.m)),
            dma((plan.u, plan.n)),
            dma((plan.u, plan.n)),
            dma((n_ta, plan.m)),
        ]
    scratch += [dma((4, 3, CHUNKS)), dma((4, 3, CHUNKS))]
    vmem = pl.BlockSpec(memory_space=pltpu.VMEM)
    anyw = pl.BlockSpec(memory_space=pl.ANY)
    result = pl.pallas_call(
        functools.partial(kernel, cfg),
        out_shape=jax.ShapeDtypeStruct((rows, model), BF16),
        in_specs=[vmem, vmem, vmem, anyw, anyw, anyw, anyw],
        out_specs=vmem,
        scratch_shapes=scratch,
        compiler_params=pltpu.CompilerParams(
            collective_id=0, has_side_effects=True, vmem_limit_bytes=67043328),
        name="axial_layer",
    )(
        tokens.reshape(rows, model),
        norm_gain,
        gains,
        jnp.transpose(qkv_weight, (0, 2, 1, 3)),
        out_weight,
        ffn_in.reshape(model, 2 * half),
        ffn_out,
    )
    return result.reshape(extent)


def solution(mesh):
    sizes = tuple(mesh.shape[name] for name in ("ta", "ha", "wa"))
    return jax.shard_map(
        functools.partial(local, sizes),
        mesh=mesh,
        in_specs=(
            P(None, "ta", "ha", "wa", None),
            P(),
            P(None, None, None, "ta"),
            P(),
            P(None, "ta", None),
            P(None, None, "ta"),
            P("ta", None),
        ),
        out_specs=P(None, "ta", "ha", "wa", None),
        check_vma=False,
    )
```
